32 devices in a mesh: kpt: 2 (over x), px: 16 (over z, y, core).
Axes of the slice: x: 2, y: 2, z: 4, core: 2. Of those that a mesh axis runs over, the one named last changes fastest.
Arguments:
- right_side: float32 [2, 3, 2, 64, 4096], P(None, None, 'kpt', 'px'), parts along dimension 2, may hold values from -6 to 6
- material: int32 [64, 4096], P('px'), may hold values from 0 to 2
- permittivity: float32 [3], replicated, may hold values from 1 to 2
- bloch_phase: float32 [6], P('kpt'), parts along dimension 0, may hold values from -3.140625 to 3.140625
- quad_shift: float32 [2], replicated, may hold values from 0.05 to 0.6, as said below
Outputs:
- solution: float32 [2, 3, 2, 64, 4096], P(None, None, 'kpt', 'px'), parts along dimension 2
- residual: float32 [2, 3, 2, 64, 4096], P(None, None, 'kpt', 'px'), parts along dimension 2
The draws below stay inside these ranges and needn't reach their ends.
There are 2 independent parts, one for each index of `kpt`. The reference program is written for one: setup_inputs(seed, part) draws one part's arguments, and reference() takes and returns one part's arrays. A program takes and returns all parts, laid end to end along the dimension named above; an argument that names none is the same for every part. Nothing has to cross between parts.
Inputs may be any that keep to these rules, and one draw needn't show every extreme that they name: quad_shift[0] lies in 0.05 to 0.1 and quad_shift[1] in 0.3 to 0.6.
All inputs are finite; a program needn't handle non-finite values.
Results may differ from the reference program's by a relative error of at most 0.0003.
Values sent between devices are 32-bit elements; how exact they have to be, the bound alone decides.
A program may use at most 128 MiB of HBM per device.

```python
import math
import jax
import jax.numpy as jnp
from jax import lax

NG = 64
VECS = 1
ITERS = 3
MATS = 3
CELLS_YZ = 4096


def draw_right_side(key, part):
    keys = jax.random.split(jax.random.fold_in(key, 11), 4)
    shape = (2, 3, VECS, NG, CELLS_YZ)
    grid_x = jnp.arange(NG, dtype=jnp.int32).astype(jnp.float32).reshape(NG, 1)
    cells = jnp.arange(CELLS_YZ, dtype=jnp.int32).reshape(1, CELLS_YZ)
    grid_y = (cells // NG).astype(jnp.float32)
    grid_z = (cells % NG).astype(jnp.float32)
    offsets = jax.random.uniform(keys[1], (3,), minval=-math.pi, maxval=math.pi)
    wave = jnp.cos(2.0 * math.pi * grid_x / NG + offsets[0]) * jnp.cos(2.0 * math.pi * grid_y / NG + offsets[1]) * jnp.cos(2.0 * math.pi * grid_z / NG + offsets[2])
    amplitude = jax.random.normal(keys[2], (2, 3, VECS, 1, 1))
    rough = jax.random.normal(keys[0], shape)
    level = jax.random.normal(keys[3], (2, 3, VECS, 1, 1))
    field = rough + level + amplitude * wave
    return jnp.clip(field, -6.0, 6.0).astype(jnp.float32)


def draw_quad_shift(key, part):
    keys = jax.random.split(jax.random.fold_in(key, 23), 2)
    real_part = jax.random.uniform(keys[0], (), minval=0.05, maxval=0.1)
    imag_part = jax.random.uniform(keys[1], (), minval=0.3, maxval=0.6)
    return jnp.stack([real_part, imag_part]).astype(jnp.float32)


def touch_ends(entries, key, low, top_value):
    dims = entries.shape
    spot = [jax.random.randint(jax.random.fold_in(key, axis), (), 0, dims[axis]) for axis in range(len(dims))]
    entries = entries.at[tuple(spot)].set(low)
    longest = dims.index(max(dims))
    spot[longest] = (spot[longest] + 1) % dims[longest]
    return entries.at[tuple(spot)].set(top_value)


def setup_inputs(seed: int = 0, part: int = 0) -> dict:
    splits = jax.random.split(jax.random.key(seed), 6)
    part_splits = jax.random.split(jax.random.fold_in(splits[5], part), 6)
    right_side = draw_right_side(jax.random.fold_in(jax.random.fold_in(splits[5], part), 71), part)
    material = touch_ends(jax.random.randint(splits[1], (NG, CELLS_YZ), 0, MATS), jax.random.fold_in(splits[1], 1), 0, MATS - 1).astype(jnp.int32)
    permittivity = jnp.clip(jnp.exp(jax.random.uniform(splits[2], (MATS,), jnp.float32, math.log(1.0), math.log(2.0))), 1.0, 2.0)
    bloch_phase = jnp.clip(jax.random.uniform(part_splits[3], (3,), jnp.float32, -3.140625, 3.140625), -3.140625, 3.140625)
    quad_shift = draw_quad_shift(jax.random.fold_in(splits[5], 71), part)
    return dict(right_side=right_side, material=material, permittivity=permittivity, bloch_phase=bloch_phase, quad_shift=quad_shift)


PRECISE = lax.Precision.HIGHEST


def block_solve(matrix_re, matrix_im, right_re, right_im):
    blocks = matrix_re.shape[0]
    system = jnp.concatenate([jnp.concatenate([matrix_re, -matrix_im], 1), jnp.concatenate([matrix_im, matrix_re], 1)], 0)
    values = jnp.concatenate([right_re, right_im], 0)
    doubled = 2 * blocks
    for pivot_row in range(doubled - 1):
        factors = system[pivot_row + 1:, pivot_row:pivot_row + 1] / system[pivot_row, pivot_row]
        system = jnp.concatenate([system[:pivot_row + 1], system[pivot_row + 1:] - factors * system[pivot_row:pivot_row + 1]], 0)
        values = jnp.concatenate([values[:pivot_row + 1], values[pivot_row + 1:] - factors * values[pivot_row:pivot_row + 1]], 0)
    rows_out = [None] * doubled
    for pivot_row in range(doubled - 1, -1, -1):
        running = values[pivot_row]
        for later_row in range(pivot_row + 1, doubled):
            running = running - system[pivot_row, later_row] * rows_out[later_row]
        rows_out[pivot_row] = running / system[pivot_row, pivot_row]
    solved = jnp.stack(rows_out, 0)
    return solved[:blocks], solved[blocks:]


def material_scale(material, permittivity):
    scaled = jnp.zeros(material.shape, jnp.float32)
    for material_id in range(permittivity.shape[0]):
        scaled = scaled + jnp.where(material == material_id, permittivity[material_id], jnp.float32(0.0))
    return scaled


def edge_weight(length_axis, along, phase_value, at_end):
    position = jnp.arange(length_axis)
    target = length_axis - 1 if at_end else 0
    weights = jnp.where(position == target, phase_value, jnp.ones((), phase_value.dtype))
    layout = tuple(length_axis if place_dim == along else 1 for place_dim in range(4))
    return weights.reshape(layout)


def forward_step(fields, along, phase_value):
    return jnp.roll(fields, -1, along) * edge_weight(fields.shape[along], along, phase_value, True) - fields


def backward_step(fields, along, phase_value):
    return jnp.roll(fields, 1, along) * edge_weight(fields.shape[along], along, jnp.conj(phase_value), False) - fields


def curl(fields, phases):
    first = forward_step(fields[2], 2, phases[1]) - forward_step(fields[1], 3, phases[2])
    second = forward_step(fields[0], 3, phases[2]) - forward_step(fields[2], 1, phases[0])
    third = forward_step(fields[1], 1, phases[0]) - forward_step(fields[0], 2, phases[1])
    return jnp.stack([first, second, third])


def curl_adjoint(fields, phases):
    first = backward_step(fields[1], 3, phases[2]) - backward_step(fields[2], 2, phases[1])
    second = backward_step(fields[2], 1, phases[0]) - backward_step(fields[0], 3, phases[2])
    third = backward_step(fields[0], 2, phases[1]) - backward_step(fields[1], 1, phases[0])
    return jnp.stack([first, second, third])


def operate(fields, inverse_eps, permit, shift_value, phases):
    return curl_adjoint(curl(fields, phases) * inverse_eps, phases) + permit * (shift_value * fields)


def precondition(fields, angles, damping):
    grid_index = jnp.arange(NG).astype(jnp.float32)
    twists = [jnp.exp(-1j * angles[which_one] * grid_index / NG) for which_one in range(3)]
    twisted = fields * twists[0].reshape(1, 1, NG, 1, 1) * twists[1].reshape(1, 1, 1, NG, 1) * twists[2].reshape(1, 1, 1, 1, NG)
    spectrum = jnp.fft.fftn(twisted, axes=(2, 3, 4))
    differences = [jnp.exp(1j * (2.0 * math.pi * grid_index + angles[which_one]) / NG) - 1.0 for which_one in range(3)]
    differences = [differences[0].reshape(1, NG, 1, 1), differences[1].reshape(1, 1, NG, 1), differences[2].reshape(1, 1, 1, NG)]
    inner_term = jnp.conj(differences[0]) * spectrum[0] + jnp.conj(differences[1]) * spectrum[1] + jnp.conj(differences[2]) * spectrum[2]
    magnitude = sum(jnp.real(differences[which_one]) ** 2 + jnp.imag(differences[which_one]) ** 2 for which_one in range(3))
    solved = jnp.stack([(spectrum[which_one] + differences[which_one] * inner_term / damping) / (magnitude + damping) for which_one in range(3)])
    returned = jnp.fft.ifftn(solved, axes=(2, 3, 4))
    return returned * jnp.conj(twists[0]).reshape(1, 1, NG, 1, 1) * jnp.conj(twists[1]).reshape(1, 1, 1, NG, 1) * jnp.conj(twists[2]).reshape(1, 1, 1, 1, NG)


def gram(left_side, right_part):
    return jnp.einsum('cvxyz,cwxyz->vw', jnp.conj(left_side), right_part, precision=PRECISE)


def mix(fields, step_coef):
    return jnp.einsum('cvxyz,vw->cwxyz', fields, step_coef, precision=PRECISE)


def reference(right_side, material, permittivity, bloch_phase, quad_shift):
    vectors = right_side.shape[2]
    residual = (right_side[0] + 1j * right_side[1]).reshape(3, vectors, NG, NG, NG)
    permit = material_scale(material, permittivity).reshape(NG, NG, NG)
    inverse_eps = 1.0 / permit
    shift_value = quad_shift[0] + 1j * quad_shift[1]
    damping = quad_shift[0] * jnp.mean(permittivity)
    phases = [jnp.exp(1j * bloch_phase[which_one]) for which_one in range(3)]
    solution = jnp.zeros_like(residual)
    direction = precondition(residual, bloch_phase, damping)
    for iteration in range(ITERS):
        image_dir = operate(direction, inverse_eps, permit, shift_value, phases)
        gram_mat = gram(direction, image_dir)
        right_mat = gram(direction, residual)
        coef_re, coef_im = block_solve(jnp.real(gram_mat), jnp.imag(gram_mat), jnp.real(right_mat), jnp.imag(right_mat))
        step_coef = coef_re + 1j * coef_im
        solution = solution + mix(direction, step_coef)
        residual = residual - mix(image_dir, step_coef)
        if iteration < ITERS - 1:
            precond = precondition(residual, bloch_phase, damping)
            update_mat = gram(image_dir, precond)
            beta_re, beta_im = block_solve(jnp.real(gram_mat), jnp.imag(gram_mat), jnp.real(update_mat), jnp.imag(update_mat))
            direction = precond + mix(direction, -(beta_re + 1j * beta_im))
    solution_out = jnp.stack([jnp.real(solution), jnp.imag(solution)]).reshape(2, 3, vectors, NG, NG * NG).astype(jnp.float32)
    residual_out = jnp.stack([jnp.real(residual), jnp.imag(residual)]).reshape(2, 3, vectors, NG, NG * NG).astype(jnp.float32)
    return (solution_out, residual_out)
```

```python
import functools
import math

import jax
import jax.numpy as jnp
from jax import lax
from jax.experimental import pallas as pl
from jax.experimental.pallas import tpu as pltpu
from jax.sharding import PartitionSpec as P

ITERS = 3
PRECISE = lax.Precision.HIGHEST
MESH = pl.DeviceIdType.MESH


def material_scale(material, permittivity):
    scaled = jnp.zeros(material.shape, jnp.float32)
    for material_id in range(permittivity.shape[0]):
        scaled = scaled + jnp.where(
            material == material_id, permittivity[material_id], jnp.float32(0.0)
        )
    return scaled


def transform_table(theta, size, forward):
    modes = lax.broadcasted_iota(jnp.int32, (size, size), 0)
    cells = lax.broadcasted_iota(jnp.int32, (size, size), 1)
    angles = (
        2.0 * math.pi * (modes * cells % size).astype(jnp.float32) / size
        + theta * cells.astype(jnp.float32) / size
    )
    if forward:
        return jnp.cos(angles), -jnp.sin(angles)
    return jnp.cos(angles).T / size, jnp.sin(angles).T / size


def right_table(table):
    real, imag = table[0].T, table[1].T
    plain = jnp.concatenate(
        [jnp.concatenate([real, imag], 1), jnp.concatenate([-imag, real], 1)], 0
    )
    turned = jnp.concatenate(
        [jnp.concatenate([-imag, real], 1), jnp.concatenate([-real, -imag], 1)], 0
    )
    return jnp.concatenate([plain, turned], 1)


def left_table(table):
    return jnp.concatenate([table[0], table[1]], 1)


def dot(a, b):
    return lax.dot_general(
        a, b, (((1,), (0,)), ((), ())), precision=PRECISE, preferred_element_type=jnp.float32
    )


def kernel_body(
    count,
    planes,
    size,
    pad,
    scal,
    right,
    permit,
    rzf,
    lyf,
    lxf,
    rzi,
    lyi,
    lxi,
    lanes,
    dx,
    gain,
    sol_out,
    res_out,
    send,
    recv,
    precond,
    direc,
    image,
    curl_buf,
    operated,
    low_permit,
    inv_low,
    inv_eps,
    low_halo,
    up_halo,
    part_send,
    part_recv,
    a2a_send_sem,
    a2a_recv_sem,
    part_send_sem,
    part_recv_sem,
    halo_send_sem,
    halo_recv_sem,
):
    me = lax.axis_index("px")
    kys = size // count
    chunk = pad * planes * kys
    half = size

    def peer(k):
        return lax.rem(me + k, count)

    barrier = pltpu.get_barrier_semaphore()

    def greet(k, carry):
        pl.semaphore_signal(
            barrier, inc=1, device_id={"px": peer(k)}, device_id_type=MESH
        )
        return carry

    lax.fori_loop(1, count, greet, 0)
    pl.semaphore_wait(barrier, count - 1)

    sign = lanes[2:3, :]
    zfa, zfb, zba, zbb = (lanes[i : i + 1, :] for i in range(3, 7))
    dz_re, dz_im = lanes[0:1, :], lanes[1:2, :]

    def turn(f):
        return pltpu.roll(f, half, f.ndim - 1) * sign

    def cmul(re, im, f):
        return re * f + im * turn(f)

    def copy_to(src, dst, ssem, rsem, target):
        return pltpu.make_async_remote_copy(
            src_ref=src,
            dst_ref=dst,
            send_sem=ssem,
            recv_sem=rsem,
            device_id={"px": target},
            device_id_type=MESH,
        )

    def rows(dev):
        return pl.ds(pl.multiple_of(dev * chunk, 8), chunk)

    def exchange_copy(e, par, k):
        return copy_to(
            send.at[e, rows(peer(k))],
            recv.at[e, rows(me)],
            a2a_send_sem.at[par, k],
            a2a_recv_sem.at[par, k],
            peer(k),
        )

    def exchange(e, par):
        def start(k, carry):
            exchange_copy(e, par, k).start()
            return carry

        def finish(k, carry):
            exchange_copy(e, par, k).wait()
            return carry

        lax.fori_loop(1, count, start, 0)
        recv[e, rows(me), :] = send[e, rows(me), :]
        lax.fori_loop(1, count, finish, 0)

    def part_copy(e, k):
        return copy_to(
            part_send.at[e],
            part_recv.at[e, me],
            part_send_sem.at[lax.rem(e, 2), k],
            part_recv_sem.at[lax.rem(e, 2), k],
            peer(k),
        )

    def part_start(e):
        def start(k, carry):
            part_copy(e, k).start()
            return carry

        lax.fori_loop(1, count, start, 0)
        part_recv[e, me] = part_send[e]

    def part_finish(e):
        def finish(k, carry):
            part_copy(e, k).wait()
            return carry

        lax.fori_loop(1, count, finish, 0)
        total = part_recv[e, 0]
        for s in range(1, count):
            total = total + part_recv[e, s]
        return jnp.sum(total, axis=1, keepdims=True)

    permit_copy = copy_to(
        permit.at[planes - 1],
        low_permit,
        halo_send_sem.at[0],
        halo_recv_sem.at[0],
        peer(1),
    )
    permit_copy.start()
    inv_eps[...] = 1.0 / permit[...]

    def halo_copies(it):
        low = copy_to(
            precond.at[it, :, planes - 1],
            low_halo.at[it],
            halo_send_sem.at[1],
            halo_recv_sem.at[1],
            peer(1),
        )
        up = copy_to(
            precond.at[it, 1:3, 0],
            up_halo.at[it],
            halo_send_sem.at[2],
            halo_recv_sem.at[2],
            lax.rem(me + count - 1, count),
        )
        return low, up

    def spectrum_forward(e):
        for c in range(3):
            for x in range(planes):
                both = dot(image[c, x], rzf[...])
                mixed = jnp.concatenate([both[:, : 2 * half], both[:, 2 * half :]], 0)
                out = dot(lyf[...], mixed)
                for d in range(count):
                    at = d * chunk + (x * pad + c) * kys
                    send[e, at : at + kys, :] = out[d * kys : (d + 1) * kys, :]

    def columns_work(e):
        for k in range(kys):
            dy_re, dy_im = scal[8 + 2 * k], scal[9 + 2 * k]
            dx_re, dx_im = dx[0], dx[1]
            spec = []
            inner = None
            factors = [(dx_re, dx_im), (dy_re, dy_im), (dz_re, dz_im)]
            for c in range(3):
                g = recv[e, pl.ds(c * kys + k, size, stride=pad * kys), :]
                w = dot(lxf[...], jnp.concatenate([g, turn(g)], 0))
                spec.append(w)
                term = factors[c][0] * w - factors[c][1] * turn(w)
                inner = term if inner is None else inner + term
            scale = gain[k]
            inner = inner * (scale * scal[6])
            inner_turned = turn(inner)
            for c in range(3):
                u = spec[c] * scale + factors[c][0] * inner + factors[c][1] * inner_turned
                out = dot(lxi[...], jnp.concatenate([u, turn(u)], 0))
                for d in range(count):
                    at = d * chunk + (k * pad + c) * planes
                    send[e + 1, at : at + planes, :] = out[d * planes : (d + 1) * planes, :]

    def field_back(e, c, x):
        v = recv[e + 1, pl.ds(c * planes + x, size, stride=pad * planes), :]
        both = dot(v, rzi[...])
        mixed = jnp.concatenate([both[:, : 2 * half], both[:, 2 * half :]], 0)
        return dot(lyi[...], mixed)

    cos_y, sin_y = scal[0], scal[1]
    cos_up, sin_up, cos_dn, sin_dn = scal[2], scal[3], scal[4], scal[5]
    q0, q1 = scal[7], scal[8 + 2 * kys]
    row = lax.broadcasted_iota(jnp.int32, (size, 2 * half), 0)

    def next_y(f):
        edge = cmul(cos_y, sin_y, f[0:1])
        return jnp.where(row == size - 1, edge, pltpu.roll(f, size - 1, 0))

    def prev_y(f):
        edge = cmul(cos_y, -sin_y, f[size - 1 : size])
        return jnp.where(row == 0, edge, pltpu.roll(f, 1, 0))

    def next_z(f):
        return pltpu.roll(f, 2 * half - 1, 1) * zfa + pltpu.roll(f, half - 1, 1) * zfb

    def prev_z(f):
        return pltpu.roll(f, 1, 1) * zba + pltpu.roll(f, half + 1, 1) * zbb

    def operate(it):
        for x in range(-1, planes):
            if x < 0:
                e = [cmul(cos_dn, sin_dn, low_halo[it, c]) for c in range(3)]
                inv = inv_low[...]
            else:
                e = [precond[it, c, x] for c in range(3)]
                inv = inv_eps[x]
            if x + 1 < planes:
                up_y, up_z = precond[it, 1, x + 1], precond[it, 2, x + 1]
            else:
                up_y, up_z = (cmul(cos_up, sin_up, up_halo[it, c]) for c in range(2))
            curl_buf[1, x + 1] = ((next_z(e[0]) - e[0]) - (up_z - e[2])) * inv
            curl_buf[2, x + 1] = ((up_y - e[1]) - (next_y(e[0]) - e[0])) * inv
            if x >= 0:
                curl_buf[0, x + 1] = (
                    (next_y(e[2]) - e[2]) - (next_z(e[1]) - e[1])
                ) * inv
        for x in range(planes):
            h = [curl_buf[c, x + 1] for c in range(3)]
            low_y, low_z = curl_buf[1, x], curl_buf[2, x]
            parts = [
                (prev_z(h[1]) - h[1]) - (prev_y(h[2]) - h[2]),
                (low_z - h[2]) - (prev_z(h[0]) - h[0]),
                (prev_y(h[0]) - h[0]) - (low_y - h[1]),
            ]
            for c in range(3):
                operated[c, x] = parts[c] + cmul(q0, q1, precond[it, c, x]) * permit[x]

    def solve(g_re, g_im, s_re, s_im):
        factor = g_im / g_re
        low = (s_im - factor * s_re) / (g_re + factor * g_im)
        return (s_re + g_im * low) / g_re, low

    def folded(value):
        return jnp.sum(value, axis=0, keepdims=True)

    image[...] = right[...]
    res_out[...] = right[...]
    sol_out[...] = jnp.zeros_like(sol_out)
    direc[...] = jnp.zeros_like(direc)

    def update(coef_re, coef_im):
        for c in range(3):
            for x in range(planes):
                sol_out[c, x] = sol_out[c, x] + cmul(coef_re, coef_im, direc[c, x])
                res_out[c, x] = res_out[c, x] - cmul(coef_re, coef_im, image[c, x])

    def gram_totals(it):
        totals = part_finish(2 * it - 1)
        return totals[0:1], totals[1:2], totals[2:3], totals[3:4]

    def iteration(it, carry):
        e = 2 * it
        spectrum_forward(e)
        exchange(e, 0)
        columns_work(e)
        exchange(e + 1, 1)

        @pl.when(it == 0)
        def _():
            for c in range(3):
                for x in range(planes):
                    precond[it, c, x] = field_back(e, c, x)
            for copy in halo_copies(it):
                copy.start()
            permit_copy.wait()
            inv_low[...] = 1.0 / low_permit[...]
            for copy in halo_copies(it):
                copy.wait()
            operate(it)
            for c in range(3):
                for x in range(planes):
                    direc[c, x] = precond[it, c, x]
                    image[c, x] = operated[c, x]

        @pl.when(it > 0)
        def _():
            g_re, g_im, s_re, s_im = gram_totals(it)
            coef_re, coef_im = solve(g_re, g_im, s_re, s_im)
            sum_re = jnp.zeros((size, 2 * half), jnp.float32)
            sum_im = jnp.zeros((size, 2 * half), jnp.float32)
            for c in range(3):
                for x in range(planes):
                    back = field_back(e, c, x)
                    value = precond[it - 1, c, x] - cmul(coef_re, coef_im, back)
                    precond[it, c, x] = value
                    sum_re = sum_re + image[c, x] * value
                    sum_im = sum_im - image[c, x] * turn(value)
            for copy in halo_copies(it):
                copy.start()
            part_send[2 * it, 0:1] = folded(sum_re)
            part_send[2 * it, 1:2] = folded(sum_im)
            part_start(2 * it)
            update(coef_re, coef_im)
            for copy in halo_copies(it):
                copy.wait()
            operate(it)
            totals = part_finish(2 * it)
            beta_re, beta_im = solve(g_re, g_im, totals[0:1], totals[1:2])
            for c in range(3):
                for x in range(planes):
                    direc[c, x] = precond[it, c, x] - cmul(beta_re, beta_im, direc[c, x])
                    image[c, x] = operated[c, x] - cmul(beta_re, beta_im, image[c, x])

        sums = [jnp.zeros((size, 2 * half), jnp.float32) for _ in range(4)]
        for c in range(3):
            for x in range(planes):
                d, m, r = direc[c, x], image[c, x], res_out[c, x]
                td = turn(d)
                sums[0] = sums[0] + d * m
                sums[1] = sums[1] + td * m
                sums[2] = sums[2] + d * r
                sums[3] = sums[3] + td * r
        for i in range(4):
            part_send[2 * it + 1, i : i + 1] = folded(sums[i])
        part_start(2 * it + 1)
        return carry

    part_send[...] = jnp.zeros_like(part_send)
    lax.fori_loop(0, ITERS, iteration, 0)
    update(*solve(*gram_totals(ITERS)))


def on_device(right_side, material, permittivity, bloch_phase, quad_shift):
    planes = right_side.shape[3]
    count = lax.axis_size("px")
    size = planes * count
    kys = size // count
    pad = 3
    while (pad * planes * kys) % 8:
        pad += 1
    position = lax.axis_index("px")
    f32 = jnp.float32

    permit = material_scale(material, permittivity).reshape(planes, size, size)
    permit = jnp.concatenate([permit, permit], 2)
    damping = quad_shift[0] * jnp.mean(permittivity)
    cosines, sines = jnp.cos(bloch_phase), jnp.sin(bloch_phase)
    is_top = position == count - 1
    is_bottom = position == 0
    modes = jnp.arange(size).astype(f32)
    kappas = [(2.0 * math.pi * modes + bloch_phase[a]) / size for a in range(3)]
    diffs = [(jnp.cos(kappa) - 1.0, jnp.sin(kappa)) for kappa in kappas]
    mine = [lax.dynamic_slice(part, (position * kys,), (kys,)) for part in diffs[1]]
    scal = jnp.concatenate(
        [
            jnp.stack(
                [
                    cosines[1],
                    sines[1],
                    jnp.where(is_top, cosines[0], 1.0),
                    jnp.where(is_top, sines[0], 0.0),
                    jnp.where(is_bottom, cosines[0], 1.0),
                    jnp.where(is_bottom, -sines[0], 0.0),
                    1.0 / damping,
                    quad_shift[0],
                ]
            ),
            jnp.stack(mine, 1).reshape(2 * kys),
            quad_shift[1:2],
        ]
    )
    squares = [re**2 + im**2 for re, im in diffs]
    mine_square = lax.dynamic_slice(squares[1], (position * kys,), (kys,))
    twice = lambda v: jnp.concatenate([v, v])
    gain = 1.0 / (
        squares[0][None, :, None]
        + mine_square[:, None, None]
        + twice(squares[2])[None, None, :]
        + damping
    )
    lane = jnp.arange(2 * size)
    low = lane < size
    last = lane % size == size - 1
    first = lane % size == 0
    lanes = jnp.stack(
        [
            twice(diffs[2][0]),
            twice(diffs[2][1]),
            jnp.where(low, -1.0, 1.0),
            jnp.where(last, jnp.where(low, -sines[2], sines[2]), 1.0),
            jnp.where(last, cosines[2], 0.0),
            jnp.where(first, jnp.where(low, sines[2], -sines[2]), 1.0),
            jnp.where(first, cosines[2], 0.0),
            jnp.zeros((2 * size,), f32),
        ]
    )
    dx = jnp.broadcast_to(jnp.stack(diffs[0])[:, :, None], (2, size, 2 * size))
    forward = [transform_table(bloch_phase[a], size, True) for a in range(3)]
    inverse = [transform_table(bloch_phase[a], size, False) for a in range(3)]
    field = right_side.reshape(2, 3, planes, size, size).transpose(1, 2, 3, 0, 4)
    field = field.reshape(3, planes, size, 2 * size)

    vmem = pl.BlockSpec(memory_space=pltpu.VMEM)
    fields = lambda n: pltpu.VMEM((3, n, size, 2 * size), f32)
    plane = (size, 2 * size)
    all_rows = count * pad * planes * kys
    dma = pltpu.SemaphoreType.DMA
    out = jax.ShapeDtypeStruct((3, planes, size, 2 * size), f32)
    solved, left = pl.pallas_call(
        functools.partial(kernel_body, count, planes, size, pad),
        out_shape=(out, out),
        in_specs=[pl.BlockSpec(memory_space=pltpu.SMEM)] + [vmem] * 11,
        out_specs=(vmem, vmem),
        scratch_shapes=[
            pltpu.VMEM((2 * ITERS, all_rows, 2 * size), f32),
            pltpu.VMEM((2 * ITERS, all_rows, 2 * size), f32),
            pltpu.VMEM((ITERS, 3, planes) + plane, f32),
            fields(planes),
            fields(planes),
            fields(planes + 1),
            fields(planes),
            pltpu.VMEM(plane, f32),
            pltpu.VMEM(plane, f32),
            pltpu.VMEM((planes,) + plane, f32),
            pltpu.VMEM((ITERS, 3) + plane, f32),
            pltpu.VMEM((ITERS, 2) + plane, f32),
            pltpu.VMEM((2 * ITERS, 8, 2 * size), f32),
            pltpu.VMEM((2 * ITERS, count, 8, 2 * size), f32),
            dma((2, count)),
            dma((2, count)),
            dma((2, count)),
            dma((2, count)),
            dma((3,)),
            dma((3,)),
        ],
        compiler_params=pltpu.CompilerParams(
            collective_id=0, has_side_effects=True, vmem_limit_bytes=60 * 2**20
        ),
    )(
        scal,
        field,
        permit,
        right_table(forward[2]),
        left_table(forward[1]),
        left_table(forward[0]),
        right_table(inverse[2]),
        left_table(inverse[1]),
        left_table(inverse[0]),
        lanes,
        dx,
        gain,
    )

    def restored(value):
        value = value.reshape(3, planes, size, 2, size).transpose(3, 0, 1, 2, 4)
        return value.reshape(right_side.shape)

    return restored(solved), restored(left)


def solution(mesh):
    return jax.shard_map(
        on_device,
        mesh=mesh,
        in_specs=(P(None, None, "kpt", "px", None), P("px", None), P(), P("kpt"), P()),
        out_specs=(P(None, None, "kpt", "px", None), P(None, None, "kpt", "px", None)),
        check_vma=False,
    )
```

```python
import functools
import math

import jax
import jax.numpy as jnp
from jax import lax
from jax.experimental import pallas as pl
from jax.experimental.pallas import tpu as pltpu
from jax.sharding import PartitionSpec as P

ITERS = 3
PRECISE = lax.Precision.HIGHEST
MESH = pl.DeviceIdType.MESH


def dot(a, b):
    return lax.dot_general(
        a, b, (((1,), (0,)), ((), ())), precision=PRECISE, preferred_element_type=jnp.float32
    )


def kernel_body(
    count,
    planes,
    size,
    pad,
    kinds,
    permittivity,
    bloch,
    shift,
    right,
    material,
    sol_flat,
    res_flat,
    sol_out,
    res_out,
    permit,
    rzf,
    lyf,
    lxf,
    rzi,
    lyi,
    lxi,
    lanes,
    dx,
    gain,
    spec,
    inner_buf,
    send,
    recv,
    precond,
    direc,
    image,
    curl_buf,
    operated,
    low_permit,
    inv_low,
    inv_eps,
    low_halo,
    up_halo,
    part_send,
    part_recv,
    a2a_send_sem,
    a2a_recv_sem,
    part_send_sem,
    part_recv_sem,
    halo_send_sem,
    halo_recv_sem,
):
    me = lax.axis_index("px")
    kys = size // count
    chunk = planes * pad
    half = size

    def peer(k):
        return lax.rem(me + k, count)

    barrier = pltpu.get_barrier_semaphore()

    def greet(k, carry):
        pl.semaphore_signal(
            barrier, inc=1, device_id={"px": peer(k)}, device_id_type=MESH
        )
        return carry

    lax.fori_loop(1, count, greet, 0)

    def turn(f):
        return pltpu.roll(f, half, f.ndim - 1) * sign

    def cmul(re, im, f):
        return re * f + im * turn(f)

    def copy_to(src, dst, ssem, rsem, target):
        return pltpu.make_async_remote_copy(
            src_ref=src,
            dst_ref=dst,
            send_sem=ssem,
            recv_sem=rsem,
            device_id={"px": target},
            device_id_type=MESH,
        )

    def rows(dev):
        return pl.ds(pl.multiple_of(dev * chunk, 8), chunk)

    def exchange_copy(e, par, c, k):
        return copy_to(
            send.at[e, c, rows(peer(k))],
            recv.at[e, c, rows(me)],
            a2a_send_sem.at[par, c, k],
            a2a_recv_sem.at[par, c, k],
            peer(k),
        )

    def exchange_start(e, par, c):
        def start(k, carry):
            exchange_copy(e, par, c, k).start()
            return carry

        lax.fori_loop(1, count, start, 0)
        recv[e, c, rows(me), :] = send[e, c, rows(me), :]

    def exchange_finish(e, par, c):
        def finish(k, carry):
            exchange_copy(e, par, c, k).wait()
            return carry

        lax.fori_loop(1, count, finish, 0)

    def part_copy(e, k):
        return copy_to(
            part_send.at[e],
            part_recv.at[e, me],
            part_send_sem.at[lax.rem(e, 2), k],
            part_recv_sem.at[lax.rem(e, 2), k],
            peer(k),
        )

    def part_start(e):
        def start(k, carry):
            part_copy(e, k).start()
            return carry

        lax.fori_loop(1, count, start, 0)
        part_recv[e, me] = part_send[e]

    def part_finish(e):
        def finish(k, carry):
            part_copy(e, k).wait()
            return carry

        lax.fori_loop(1, count, finish, 0)
        total = part_recv[e, 0]
        for s in range(1, count):
            total = total + part_recv[e, s]
        return jnp.sum(total, axis=1, keepdims=True)


    wide = (size, 2 * half)
    row = lax.broadcasted_iota(jnp.int32, wide, 0)
    lane = lax.broadcasted_iota(jnp.int32, wide, 1)
    low = lane < half
    index = jnp.where(low, lane, lane - half)
    quarter = jnp.where(low, 0.0, 0.5 * math.pi)
    minus_high = jnp.where(low, 1.0, -1.0)
    minus_low = -minus_high
    base = (2.0 * math.pi / size) * lax.rem(row * index, size).astype(jnp.float32) - quarter
    sign = minus_low[0:1]

    def swap(f):
        return pltpu.roll(f, half, 1)

    def by_mode(axis):
        return jnp.cos(base + bloch[axis] * index.astype(jnp.float32) / size)

    def by_cell(axis):
        return jnp.cos(base + bloch[axis] * row.astype(jnp.float32) / size)

    lxf[...] = by_mode(0) * minus_high
    lyf[...] = by_mode(1) * minus_high
    lxi[...] = by_cell(0) / size
    lyi[...] = by_cell(1) / size
    cells = by_cell(2)
    rzf[0:half, 0 : 2 * half] = cells * minus_high
    rzf[0:half, 2 * half :] = swap(cells)
    rzf[half:, 0 : 2 * half] = swap(cells)
    rzf[half:, 2 * half :] = cells * minus_low
    modes = by_mode(2) / size
    rzi[0:half, 0 : 2 * half] = modes
    rzi[0:half, 2 * half :] = swap(modes) * minus_low
    rzi[half:, 0 : 2 * half] = swap(modes) * minus_low
    rzi[half:, 2 * half :] = -modes

    kappa_x = (2.0 * math.pi * row.astype(jnp.float32) + bloch[0]) / size
    dx[0] = jnp.cos(kappa_x) - 1.0
    dx[1] = jnp.sin(kappa_x)
    short = (lanes.shape[1], 2 * half)
    line = lax.broadcasted_iota(jnp.int32, short, 0)
    place = lax.broadcasted_iota(jnp.int32, short, 1)
    place = jnp.where(place < half, place, place - half)
    angles = (2.0 * math.pi * place.astype(jnp.float32) + bloch[2]) / size
    for axis in range(3):
        angles = jnp.where(line == axis, bloch[axis], angles)
    for k in range(kys):
        ky = (me * kys + k).astype(jnp.float32)
        angles = jnp.where(line == 4 + k, (2.0 * math.pi * ky + bloch[1]) / size, angles)
    lanes[0] = jnp.cos(angles)
    lanes[1] = jnp.sin(angles)

    def wave(i):
        return lanes[0, i : i + 1, :], lanes[1, i : i + 1, :]

    def difference(i):
        return lanes[0, i : i + 1, :] - 1.0, lanes[1, i : i + 1, :]

    mean = permittivity[0]
    for i in range(1, kinds):
        mean = mean + permittivity[i]
    damping = jnp.full((1, 2 * half), shift[0] * mean * (1.0 / kinds), jnp.float32)
    over_damping = 1.0 / damping
    dz_re, dz_im = difference(3)
    square_z = dz_re**2 + dz_im**2
    square_x = dx[0] ** 2 + dx[1] ** 2
    for k in range(kys):
        dy_re, dy_im = difference(4 + k)
        gain[k] = 1.0 / (square_x + (dy_re**2 + dy_im**2) + square_z + damping)

    (cos_x, sin_x), (cos_y, sin_y), (cos_z, sin_z) = (wave(axis) for axis in range(3))
    cos_up = jnp.where(me == count - 1, cos_x, 1.0)
    sin_up = jnp.where(me == count - 1, sin_x, 0.0)
    cos_dn = jnp.where(me == 0, cos_x, 1.0)
    sin_dn = jnp.where(me == 0, -sin_x, 0.0)
    index_row, low_row = index[0:1], low[0:1]
    last, first = index_row == size - 1, index_row == 0
    zfa = jnp.where(last, jnp.where(low_row, -sin_z, sin_z), 1.0)
    zfb = jnp.where(last, cos_z, 0.0)
    zba = jnp.where(first, jnp.where(low_row, sin_z, -sin_z), 1.0)
    zbb = jnp.where(first, cos_z, 0.0)
    q0, q1 = shift[0], shift[1]

    half_low = low[0 : size // 2]

    def every(x):
        return pl.ds(x, size // 2, stride=planes)

    even, odd = pl.ds(0, size // 2, stride=2), pl.ds(1, size // 2, stride=2)
    for x in range(planes):
        kind = material[every(x), :]
        scaled = jnp.zeros(kind.shape, jnp.float32)
        for i in range(kinds):
            scaled = scaled + jnp.where(kind == i, permittivity[i], jnp.float32(0.0))
        turned = swap(scaled)
        permit[x, even, :] = jnp.where(half_low, scaled, turned)
        permit[x, odd, :] = jnp.where(half_low, turned, scaled)
        for c in range(3):
            re, im = right[0, c, every(x), :], right[1, c, every(x), :]
            res_out[c, x, even, :] = jnp.where(half_low, re, swap(im))
            res_out[c, x, odd, :] = jnp.where(half_low, swap(re), im)

    def emit(flat, field, c, x):
        a, b = field[c, x, even, :], field[c, x, odd, :]
        flat[0, c, every(x), :] = jnp.where(half_low, a, swap(b))
        flat[1, c, every(x), :] = jnp.where(half_low, swap(a), b)

    pl.semaphore_wait(barrier, count - 1)

    permit_copy = copy_to(
        permit.at[planes - 1],
        low_permit,
        halo_send_sem.at[0],
        halo_recv_sem.at[0],
        peer(1),
    )
    permit_copy.start()
    inv_eps[...] = 1.0 / permit[...]

    def halo_copies(it):
        low = copy_to(
            precond.at[it, :, planes - 1],
            low_halo.at[it],
            halo_send_sem.at[1],
            halo_recv_sem.at[1],
            peer(1),
        )
        up = copy_to(
            precond.at[it, 1:3, 0],
            up_halo.at[it],
            halo_send_sem.at[2],
            halo_recv_sem.at[2],
            lax.rem(me + count - 1, count),
        )
        return low, up

    def spectrum_forward(e, c):
        for x in range(planes):
            both = dot(image[c, x], rzf[...])
            mixed = jnp.concatenate([both[:, : 2 * half], both[:, 2 * half :]], 0)
            out = dot(lyf[...], mixed)
            for d in range(count):
                at = d * chunk + x * pad
                send[e, c, at : at + kys, :] = out[d * kys : (d + 1) * kys, :]

    def symbol(k):
        return [(dx[0], dx[1]), difference(4 + k), difference(3)]

    def columns_in(e, c):
        for k in range(kys):
            g = recv[e, c, pl.ds(k, size, stride=pad), :]
            w = dot(lxf[...], jnp.concatenate([g, turn(g)], 0))
            spec[c, k] = w
            re, im = symbol(k)[c]
            term = re * w - im * turn(w)
            if c == 0:
                inner_buf[k] = term
            elif c == 1:
                inner_buf[k] = inner_buf[k] + term
            else:
                inner_buf[k] = (inner_buf[k] + term) * (gain[k] * over_damping)

    def columns_out(e, c):
        for k in range(kys):
            re, im = symbol(k)[c]
            u = spec[c, k] * gain[k] + cmul(re, im, inner_buf[k])
            out = dot(lxi[...], jnp.concatenate([u, turn(u)], 0))
            for d in range(count):
                at = d * chunk + k * pad
                send[e + 1, c, at : at + planes, :] = out[d * planes : (d + 1) * planes, :]

    def field_back(e, c, x):
        v = recv[e + 1, c, pl.ds(x, size, stride=pad), :]
        both = dot(v, rzi[...])
        mixed = jnp.concatenate([both[:, : 2 * half], both[:, 2 * half :]], 0)
        return dot(lyi[...], mixed)

    def next_y(f):
        edge = cmul(cos_y, sin_y, f[0:1])
        return jnp.where(row == size - 1, edge, pltpu.roll(f, size - 1, 0))

    def prev_y(f):
        edge = cmul(cos_y, -sin_y, f[size - 1 : size])
        return jnp.where(row == 0, edge, pltpu.roll(f, 1, 0))

    def next_z(f):
        return pltpu.roll(f, 2 * half - 1, 1) * zfa + pltpu.roll(f, half - 1, 1) * zfb

    def prev_z(f):
        return pltpu.roll(f, 1, 1) * zba + pltpu.roll(f, half + 1, 1) * zbb

    def operate(it):
        for x in range(-1, planes):
            if x < 0:
                e = [cmul(cos_dn, sin_dn, low_halo[it, c]) for c in range(3)]
                inv = inv_low[...]
            else:
                e = [precond[it, c, x] for c in range(3)]
                inv = inv_eps[x]
            if x + 1 < planes:
                up_y, up_z = precond[it, 1, x + 1], precond[it, 2, x + 1]
            else:
                up_y, up_z = (cmul(cos_up, sin_up, up_halo[it, c]) for c in range(2))
            curl_buf[1, x + 1] = ((next_z(e[0]) - e[0]) - (up_z - e[2])) * inv
            curl_buf[2, x + 1] = ((up_y - e[1]) - (next_y(e[0]) - e[0])) * inv
            if x >= 0:
                curl_buf[0, x + 1] = (
                    (next_y(e[2]) - e[2]) - (next_z(e[1]) - e[1])
                ) * inv
        for x in range(planes):
            h = [curl_buf[c, x + 1] for c in range(3)]
            low_y, low_z = curl_buf[1, x], curl_buf[2, x]
            parts = [
                (prev_z(h[1]) - h[1]) - (prev_y(h[2]) - h[2]),
                (low_z - h[2]) - (prev_z(h[0]) - h[0]),
                (prev_y(h[0]) - h[0]) - (low_y - h[1]),
            ]
            for c in range(3):
                operated[c, x] = parts[c] + cmul(q0, q1, precond[it, c, x]) * permit[x]

    def solve(g_re, g_im, s_re, s_im):
        factor = g_im / g_re
        low = (s_im - factor * s_re) / (g_re + factor * g_im)
        return (s_re + g_im * low) / g_re, low

    def folded(value):
        return jnp.sum(value, axis=0, keepdims=True)

    image[...] = res_out[...]
    sol_out[...] = jnp.zeros_like(sol_out)
    direc[...] = jnp.zeros_like(direc)

    def update(coef_re, coef_im):
        for c in range(3):
            for x in range(planes):
                sol_out[c, x] = sol_out[c, x] + cmul(coef_re, coef_im, direc[c, x])
                res_out[c, x] = res_out[c, x] - cmul(coef_re, coef_im, image[c, x])

    def gram_totals(it):
        totals = part_finish(2 * it - 1)
        return totals[0:1], totals[1:2], totals[2:3], totals[3:4]

    def iteration(it, carry):
        e = 2 * it
        for c in range(3):
            spectrum_forward(e, c)
            exchange_start(e, 0, c)
        for c in range(3):
            exchange_finish(e, 0, c)
            columns_in(e, c)
        for c in range(3):
            columns_out(e, c)
            exchange_start(e + 1, 1, c)

        @pl.when(it == 0)
        def _():
            for c in range(3):
                exchange_finish(e + 1, 1, c)
                for x in range(planes):
                    precond[it, c, x] = field_back(e, c, x)
            for copy in halo_copies(it):
                copy.start()
            permit_copy.wait()
            inv_low[...] = 1.0 / low_permit[...]
            for copy in halo_copies(it):
                copy.wait()
            operate(it)
            for c in range(3):
                for x in range(planes):
                    direc[c, x] = precond[it, c, x]
                    image[c, x] = operated[c, x]

        @pl.when(it > 0)
        def _():
            g_re, g_im, s_re, s_im = gram_totals(it)
            coef_re, coef_im = solve(g_re, g_im, s_re, s_im)
            sum_re = jnp.zeros((size, 2 * half), jnp.float32)
            sum_im = jnp.zeros((size, 2 * half), jnp.float32)
            for c in range(3):
                exchange_finish(e + 1, 1, c)
                for x in range(planes):
                    back = field_back(e, c, x)
                    value = precond[it - 1, c, x] - cmul(coef_re, coef_im, back)
                    precond[it, c, x] = value
                    sum_re = sum_re + image[c, x] * value
                    sum_im = sum_im - image[c, x] * turn(value)
            for copy in halo_copies(it):
                copy.start()
            part_send[2 * it, 0:1] = folded(sum_re)
            part_send[2 * it, 1:2] = folded(sum_im)
            part_start(2 * it)
            update(coef_re, coef_im)
            for copy in halo_copies(it):
                copy.wait()
            operate(it)
            totals = part_finish(2 * it)
            beta_re, beta_im = solve(g_re, g_im, totals[0:1], totals[1:2])
            for c in range(3):
                for x in range(planes):
                    direc[c, x] = precond[it, c, x] - cmul(beta_re, beta_im, direc[c, x])
                    image[c, x] = operated[c, x] - cmul(beta_re, beta_im, image[c, x])

        sums = [jnp.zeros((size, 2 * half), jnp.float32) for _ in range(4)]
        for c in range(3):
            for x in range(planes):
                d, m, r = direc[c, x], image[c, x], res_out[c, x]
                td = turn(d)
                sums[0] = sums[0] + d * m
                sums[1] = sums[1] + td * m
                sums[2] = sums[2] + d * r
                sums[3] = sums[3] + td * r
        for i in range(4):
            part_send[2 * it + 1, i : i + 1] = folded(sums[i])
        part_start(2 * it + 1)
        return carry

    part_send[...] = jnp.zeros_like(part_send)
    lax.fori_loop(0, ITERS, iteration, 0)
    update(*solve(*gram_totals(ITERS)))
    for c in range(3):
        for x in range(planes):
            emit(sol_flat, sol_out, c, x)
            emit(res_flat, res_out, c, x)


def on_device(right_side, material, permittivity, bloch_phase, quad_shift):
    planes = right_side.shape[3]
    count = lax.axis_size("px")
    size = planes * count
    lanes = 2 * size
    groups = size // 2
    pad = planes
    while (planes * pad) % 8:
        pad += 1
    f32 = jnp.float32

    def flat(value):
        lead = value.shape[:-2]
        value = value.reshape(lead + (planes, groups, lanes))
        return jnp.swapaxes(value, -3, -2).reshape(lead + (groups * planes, lanes))

    def restored(value):
        value = value.reshape(2, 3, groups, planes, lanes)
        return jnp.swapaxes(value, -3, -2).reshape(right_side.shape)

    vmem = pl.BlockSpec(memory_space=pltpu.VMEM)
    smem = pl.BlockSpec(memory_space=pltpu.SMEM)
    plane = (size, lanes)
    field = pltpu.VMEM((3, planes) + plane, f32)
    planar = pltpu.VMEM((planes,) + plane, f32)
    exchanged = pltpu.VMEM((2 * ITERS, 3, count * planes * pad, lanes), f32)
    dma = pltpu.SemaphoreType.DMA
    out = jax.ShapeDtypeStruct((2, 3, groups * planes, lanes), f32)
    solved, left = pl.pallas_call(
        functools.partial(kernel_body, count, planes, size, pad, permittivity.shape[0]),
        out_shape=(out, out),
        in_specs=[smem] * 3 + [vmem] * 2,
        out_specs=(vmem, vmem),
        scratch_shapes=[
            field,
            field,
            planar,
            pltpu.VMEM((lanes, 2 * lanes), f32),
            pltpu.VMEM(plane, f32),
            pltpu.VMEM(plane, f32),
            pltpu.VMEM((lanes, 2 * lanes), f32),
            pltpu.VMEM(plane, f32),
            pltpu.VMEM(plane, f32),
            pltpu.VMEM((2, -(-(4 + planes) // 8) * 8, lanes), f32),
            pltpu.VMEM((2,) + plane, f32),
            planar,
            field,
            planar,
            exchanged,
            exchanged,
            pltpu.VMEM((ITERS, 3, planes) + plane, f32),
            field,
            field,
            pltpu.VMEM((3, planes + 1) + plane, f32),
            field,
            pltpu.VMEM(plane, f32),
            pltpu.VMEM(plane, f32),
            planar,
            pltpu.VMEM((ITERS, 3) + plane, f32),
            pltpu.VMEM((ITERS, 2) + plane, f32),
            pltpu.VMEM((2 * ITERS, 8, lanes), f32),
            pltpu.VMEM((2 * ITERS, count, 8, lanes), f32),
            dma((2, 3, count)),
            dma((2, 3, count)),
            dma((2, count)),
            dma((2, count)),
            dma((3,)),
            dma((3,)),
        ],
        compiler_params=pltpu.CompilerParams(
            collective_id=0, has_side_effects=True, vmem_limit_bytes=60 * 2**20
        ),
    )(permittivity, bloch_phase, quad_shift, flat(right_side[:, :, 0]), flat(material))
    return restored(solved), restored(left)


def solution(mesh):
    return jax.shard_map(
        on_device,
        mesh=mesh,
        in_specs=(P(None, None, "kpt", "px", None), P("px", None), P(), P("kpt"), P()),
        out_specs=(P(None, None, "kpt", "px", None), P(None, None, "kpt", "px", None)),
        check_vma=False,
    )
```

```python
import functools
import math

import jax
import jax.numpy as jnp
from jax import lax
from jax.experimental import pallas as pl
from jax.experimental.pallas import tpu as pltpu
from jax.sharding import PartitionSpec as P

ITERS = 3
PRECISE = lax.Precision.HIGHEST
MESH = pl.DeviceIdType.MESH


def dot(a, b):
    return lax.dot_general(
        a, b, (((1,), (0,)), ((), ())), precision=PRECISE, preferred_element_type=jnp.float32
    )


def kernel_body(
    count,
    planes,
    size,
    pad,
    kinds,
    permittivity,
    bloch,
    shift,
    right,
    material,
    sol_flat,
    res_flat,
    sol_out,
    res_out,
    permit,
    rzf,
    lyf,
    rzi,
    lyi,
    lanes,
    dy,
    decay,
    green,
    middle,
    own_decay,
    wrap,
    spec,
    solved,
    inner_buf,
    low_spec,
    send,
    recv,
    precond,
    direc,
    image,
    curl_buf,
    operated,
    low_permit,
    inv_low,
    inv_eps,
    part_send,
    part_recv,
    a2a_send_sem,
    a2a_recv_sem,
    part_send_sem,
    part_recv_sem,
    halo_send_sem,
    halo_recv_sem,
):
    me = lax.axis_index("px")
    kys = size // count
    chunk = pad
    half = size

    def peer(k):
        return lax.rem(me + k, count)

    barrier = pltpu.get_barrier_semaphore()

    def greet(k, carry):
        pl.semaphore_signal(
            barrier, inc=1, device_id={"px": peer(k)}, device_id_type=MESH
        )
        return carry

    lax.fori_loop(1, count, greet, 0)

    def turn(f):
        return pltpu.roll(f, half, f.ndim - 1) * sign

    def cmul(re, im, f):
        return re * f + im * turn(f)

    def copy_to(src, dst, ssem, rsem, target):
        return pltpu.make_async_remote_copy(
            src_ref=src,
            dst_ref=dst,
            send_sem=ssem,
            recv_sem=rsem,
            device_id={"px": target},
            device_id_type=MESH,
        )

    def rows(dev):
        return pl.ds(pl.multiple_of(dev * chunk, 8), chunk)

    def exchange_copy(e, par, c, k):
        return copy_to(
            send.at[e, c, rows(peer(k))],
            recv.at[e, c, rows(me)],
            a2a_send_sem.at[par, c, k],
            a2a_recv_sem.at[par, c, k],
            peer(k),
        )

    def exchange_start(e, par, c):
        def start(k, carry):
            exchange_copy(e, par, c, k).start()
            return carry

        lax.fori_loop(1, count, start, 0)
        recv[e, c, rows(me), :] = send[e, c, rows(me), :]

    def exchange_finish(e, par, c):
        def finish(k, carry):
            exchange_copy(e, par, c, k).wait()
            return carry

        lax.fori_loop(1, count, finish, 0)

    def part_copy(e, k):
        return copy_to(
            part_send.at[e],
            part_recv.at[e, me],
            part_send_sem.at[lax.rem(e, 2), k],
            part_recv_sem.at[lax.rem(e, 2), k],
            peer(k),
        )

    def part_start(e):
        def start(k, carry):
            part_copy(e, k).start()
            return carry

        lax.fori_loop(1, count, start, 0)
        part_recv[e, me] = part_send[e]

    def part_finish(e):
        def finish(k, carry):
            part_copy(e, k).wait()
            return carry

        lax.fori_loop(1, count, finish, 0)
        total = part_recv[e, 0]
        for s in range(1, count):
            total = total + part_recv[e, s]
        return jnp.sum(total, axis=1, keepdims=True)


    wide = (size, 2 * half)
    row = lax.broadcasted_iota(jnp.int32, wide, 0)
    lane = lax.broadcasted_iota(jnp.int32, wide, 1)
    low = lane < half
    index = jnp.where(low, lane, lane - half)
    quarter = jnp.where(low, 0.0, 0.5 * math.pi)
    minus_high = jnp.where(low, 1.0, -1.0)
    minus_low = -minus_high
    base = (2.0 * math.pi / size) * lax.rem(row * index, size).astype(jnp.float32) - quarter
    sign = minus_low[0:1]

    def swap(f):
        return pltpu.roll(f, half, 1)

    def by_mode(axis):
        return jnp.cos(base + bloch[axis] * index.astype(jnp.float32) / size)

    def by_cell(axis):
        return jnp.cos(base + bloch[axis] * row.astype(jnp.float32) / size)

    lyf[...] = by_mode(1) * minus_high
    lyi[...] = by_cell(1) / size
    cells = by_cell(2)
    rzf[0:half, 0 : 2 * half] = cells * minus_high
    rzf[0:half, 2 * half :] = swap(cells)
    rzf[half:, 0 : 2 * half] = swap(cells)
    rzf[half:, 2 * half :] = cells * minus_low
    modes = by_mode(2) / size
    rzi[0:half, 0 : 2 * half] = modes
    rzi[0:half, 2 * half :] = swap(modes) * minus_low
    rzi[half:, 0 : 2 * half] = swap(modes) * minus_low
    rzi[half:, 2 * half :] = -modes

    kappa_y = (2.0 * math.pi * row.astype(jnp.float32) + bloch[1]) / size
    dy[0] = jnp.cos(kappa_y) - 1.0
    dy[1] = jnp.sin(kappa_y)
    short = (lanes.shape[1], 2 * half)
    line = lax.broadcasted_iota(jnp.int32, short, 0)
    place = lax.broadcasted_iota(jnp.int32, short, 1)
    place = jnp.where(place < half, place, place - half)
    angles = (2.0 * math.pi * place.astype(jnp.float32) + bloch[2]) / size
    for axis in range(3):
        angles = jnp.where(line == axis, bloch[axis], angles)
    my_ky = (me * kys + lax.rem(line, kys)).astype(jnp.float32)
    my_kappa = (2.0 * math.pi * my_ky + bloch[1]) / size
    lanes[0] = jnp.cos(angles)
    lanes[1] = jnp.sin(angles)

    def wave(i):
        return lanes[0, i : i + 1, :], lanes[1, i : i + 1, :]

    def difference(i):
        return lanes[0, i : i + 1, :] - 1.0, lanes[1, i : i + 1, :]

    mean = permittivity[0]
    for i in range(1, kinds):
        mean = mean + permittivity[i]
    damping = jnp.full((1, 2 * half), shift[0] * mean * (1.0 / kinds), jnp.float32)
    over_damping = 1.0 / damping
    dz_re, dz_im = difference(3)
    square_z = dz_re**2 + dz_im**2 + damping

    def decay_of(sigma):
        root = jnp.sqrt(sigma + 0.25 * sigma * sigma)
        return 1.0 / (1.0 + 0.5 * sigma + root), 0.5 / root

    sigma = dy[0] ** 2 + dy[1] ** 2 + square_z
    lam, green_value = decay_of(sigma)
    decay[...] = lam
    green[...] = green_value
    middle[...] = 2.0 + sigma
    my_square = (jnp.cos(my_kappa) - 1.0) ** 2 + jnp.sin(my_kappa) ** 2
    my_lam, _ = decay_of(my_square + square_z)
    my_step = my_lam
    for _ in range(planes - 1):
        my_step = my_step * my_lam
    power = jnp.ones(short, jnp.float32)
    for s in range(count):
        own_decay[s] = power
        power = power * my_step
    own_decay[count] = power
    is_low = line < kys
    cos_x, sin_x = wave(0)
    bottom = 1.0 / (1.0 - 2.0 * power * cos_x + power * power)
    wrap[0] = (cos_x - power) * bottom
    wrap[1] = jnp.where(is_low, -sin_x, sin_x) * bottom

    (cos_y, sin_y), (cos_z, sin_z) = wave(1), wave(2)
    cos_dn = jnp.where(me == 0, cos_x, 1.0)
    sin_dn = jnp.where(me == 0, -sin_x, 0.0)
    index_row, low_row = index[0:1], low[0:1]
    last, first = index_row == size - 1, index_row == 0
    zfa = jnp.where(last, jnp.where(low_row, -sin_z, sin_z), 1.0)
    zfb = jnp.where(last, cos_z, 0.0)
    zba = jnp.where(first, jnp.where(low_row, sin_z, -sin_z), 1.0)
    zbb = jnp.where(first, cos_z, 0.0)
    q0, q1 = shift[0], shift[1]

    half_low = low[0 : size // 2]

    def every(x):
        return pl.ds(x, size // 2, stride=planes)

    even, odd = pl.ds(0, size // 2, stride=2), pl.ds(1, size // 2, stride=2)
    for x in range(planes):
        kind = material[every(x), :]
        scaled = jnp.zeros(kind.shape, jnp.float32)
        for i in range(kinds):
            scaled = scaled + jnp.where(kind == i, permittivity[i], jnp.float32(0.0))
        turned = swap(scaled)
        permit[x, even, :] = jnp.where(half_low, scaled, turned)
        permit[x, odd, :] = jnp.where(half_low, turned, scaled)
        for c in range(3):
            re, im = right[0, c, every(x), :], right[1, c, every(x), :]
            res_out[c, x, even, :] = jnp.where(half_low, re, swap(im))
            res_out[c, x, odd, :] = jnp.where(half_low, swap(re), im)

    def emit(flat, field, c, x):
        a, b = field[c, x, even, :], field[c, x, odd, :]
        flat[0, c, every(x), :] = jnp.where(half_low, a, swap(b))
        flat[1, c, every(x), :] = jnp.where(half_low, swap(a), b)

    pl.semaphore_wait(barrier, count - 1)

    permit_copy = copy_to(
        permit.at[planes - 1],
        low_permit,
        halo_send_sem.at[0],
        halo_recv_sem.at[0],
        peer(1),
    )
    permit_copy.start()
    inv_eps[...] = 1.0 / permit[...]

    def plane_copy(it):
        return copy_to(
            spec.at[0, planes - 1],
            low_spec.at[it],
            halo_send_sem.at[1 + it],
            halo_recv_sem.at[1 + it],
            peer(1),
        )

    def spectrum_forward(e, c):
        lam = decay[...]
        up = down = None
        for x in range(planes):
            both = dot(image[c, x], rzf[...])
            mixed = jnp.concatenate([both[:, : 2 * half], both[:, 2 * half :]], 0)
            out = dot(lyf[...], mixed)
            spec[c, x] = out
            if x == 0:
                up = down = out
                power = lam
            else:
                up = up * lam + out
                down = down + out * power
                power = power * lam
        for d in range(count):
            at = d * chunk
            send[e, c, at : at + kys, :] = up[d * kys : (d + 1) * kys, :]
            send[e, c, at + kys : at + 2 * kys, :] = down[d * kys : (d + 1) * kys, :]

    def scan(e, c):
        step = own_decay[1]
        below, above = [jnp.zeros(short, jnp.float32)], [jnp.zeros(short, jnp.float32)]
        for s in range(count):
            t = count - 1 - s
            below.append(below[-1] * step + recv[e, c, s * chunk : (s + 1) * chunk, :])
            above.append(above[-1] * step + recv[e, c, t * chunk : (t + 1) * chunk, :])
        total = cmul(wrap[0], wrap[1], jnp.where(is_low, below[-1], above[-1]))
        for d in range(count):
            t = count - 1 - d
            value = jnp.where(is_low, below[d], above[t])
            power = jnp.where(is_low, own_decay[d], own_decay[t])
            send[e + 1, c, d * chunk : (d + 1) * chunk, :] = value + power * total

    def column_solve(e, c):
        for s in range(count):
            at = s * chunk
            inner_buf[0, s * kys : (s + 1) * kys, :] = recv[e + 1, c, at : at + kys, :]
            inner_buf[1, s * kys : (s + 1) * kys, :] = recv[
                e + 1, c, at + kys : at + 2 * kys, :
            ]
        lam, scale = decay[...], green[...]
        total = inner_buf[0]
        solved[c, 0] = total
        for x in range(planes):
            total = total * lam + spec[c, x]
            solved[c, x + 1] = total
        total = inner_buf[1]
        solved[c, planes + 1] = (solved[c, planes] * lam + total) * scale
        for x in range(planes - 1, -2, -1):
            total = total * lam
            solved[c, x + 1] = (solved[c, x + 1] + total) * scale
            if x >= 0:
                total = total + spec[c, x]

    def couple(it):
        dy_re, dy_im = dy[0], dy[1]
        low = cmul(cos_dn, sin_dn, low_spec[it])
        prior = middle[...] * solved[0, 0] - solved[0, 1] - low
        for x in range(planes + 2):
            here = solved[0, x]
            term = prior - here
            prior = here
            for c, (re, im) in ((1, (dy_re, dy_im)), (2, difference(3))):
                f = solved[c, x]
                term = term + re * f - im * turn(f)
            inner_buf[x] = term * over_damping
        for x in range(planes + 2):
            if x <= planes:
                solved[0, x] = solved[0, x] + (inner_buf[x + 1] - inner_buf[x])
            inner = inner_buf[x]
            turned = turn(inner)
            solved[1, x] = solved[1, x] + dy_re * inner + dy_im * turned
            dz_re, dz_im = difference(3)
            solved[2, x] = solved[2, x] + dz_re * inner + dz_im * turned

    def field_back(c, x):
        both = dot(solved[c, x], rzi[...])
        mixed = jnp.concatenate([both[:, : 2 * half], both[:, 2 * half :]], 0)
        return dot(lyi[...], mixed)

    def wide_planes(c):
        return planes + (1 if c == 0 else 2)

    def next_y(f):
        edge = cmul(cos_y, sin_y, f[0:1])
        return jnp.where(row == size - 1, edge, pltpu.roll(f, size - 1, 0))

    def prev_y(f):
        edge = cmul(cos_y, -sin_y, f[size - 1 : size])
        return jnp.where(row == 0, edge, pltpu.roll(f, 1, 0))

    def next_z(f):
        return pltpu.roll(f, 2 * half - 1, 1) * zfa + pltpu.roll(f, half - 1, 1) * zfb

    def prev_z(f):
        return pltpu.roll(f, 1, 1) * zba + pltpu.roll(f, half + 1, 1) * zbb

    def operate():
        for x in range(-1, planes):
            e = [precond[c, x + 1] for c in range(3)]
            inv = inv_low[...] if x < 0 else inv_eps[x]
            up_y, up_z = precond[1, x + 2], precond[2, x + 2]
            curl_buf[1, x + 1] = ((next_z(e[0]) - e[0]) - (up_z - e[2])) * inv
            curl_buf[2, x + 1] = ((up_y - e[1]) - (next_y(e[0]) - e[0])) * inv
            if x >= 0:
                curl_buf[0, x + 1] = (
                    (next_y(e[2]) - e[2]) - (next_z(e[1]) - e[1])
                ) * inv
        for x in range(planes):
            h = [curl_buf[c, x + 1] for c in range(3)]
            low_y, low_z = curl_buf[1, x], curl_buf[2, x]
            parts = [
                (prev_z(h[1]) - h[1]) - (prev_y(h[2]) - h[2]),
                (low_z - h[2]) - (prev_z(h[0]) - h[0]),
                (prev_y(h[0]) - h[0]) - (low_y - h[1]),
            ]
            for c in range(3):
                operated[c, x] = parts[c] + cmul(q0, q1, precond[c, x + 1]) * permit[x]

    def solve(g_re, g_im, s_re, s_im):
        factor = g_im / g_re
        low = (s_im - factor * s_re) / (g_re + factor * g_im)
        return (s_re + g_im * low) / g_re, low

    def folded(value):
        return jnp.sum(value, axis=0, keepdims=True)

    image[...] = res_out[...]
    sol_out[...] = jnp.zeros_like(sol_out)
    direc[...] = jnp.zeros_like(direc)

    def update(coef_re, coef_im):
        for c in range(3):
            for x in range(planes):
                sol_out[c, x] = sol_out[c, x] + cmul(coef_re, coef_im, direc[c, x])
                res_out[c, x] = res_out[c, x] - cmul(coef_re, coef_im, image[c, x])

    def gram_totals(it):
        totals = part_finish(2 * it - 1)
        return totals[0:1], totals[1:2], totals[2:3], totals[3:4]

    def iteration(it, carry):
        e = 2 * it
        for c in range(3):
            spectrum_forward(e, c)
            exchange_start(e, 0, c)
            if c == 0:
                plane_copy(it).start()
        for c in range(3):
            exchange_finish(e, 0, c)
            scan(e, c)
            exchange_start(e + 1, 1, c)
        for c in range(3):
            exchange_finish(e + 1, 1, c)
            column_solve(e, c)
        plane_copy(it).wait()
        couple(it)

        @pl.when(it == 0)
        def _():
            for c in range(3):
                for x in range(wide_planes(c)):
                    precond[c, x] = field_back(c, x)
            permit_copy.wait()
            inv_low[...] = 1.0 / low_permit[...]
            operate()
            for c in range(3):
                for x in range(planes):
                    direc[c, x] = precond[c, x + 1]
                    image[c, x] = operated[c, x]

        @pl.when(it > 0)
        def _():
            g_re, g_im, s_re, s_im = gram_totals(it)
            coef_re, coef_im = solve(g_re, g_im, s_re, s_im)
            sum_re = jnp.zeros((size, 2 * half), jnp.float32)
            sum_im = jnp.zeros((size, 2 * half), jnp.float32)
            for c in range(3):
                for x in range(wide_planes(c)):
                    value = precond[c, x] - cmul(coef_re, coef_im, field_back(c, x))
                    precond[c, x] = value
                    if 1 <= x <= planes:
                        sum_re = sum_re + image[c, x - 1] * value
                        sum_im = sum_im - image[c, x - 1] * turn(value)
            part_send[2 * it, 0:1] = folded(sum_re)
            part_send[2 * it, 1:2] = folded(sum_im)
            part_start(2 * it)
            update(coef_re, coef_im)
            operate()
            totals = part_finish(2 * it)
            beta_re, beta_im = solve(g_re, g_im, totals[0:1], totals[1:2])
            for c in range(3):
                for x in range(planes):
                    direc[c, x] = precond[c, x + 1] - cmul(beta_re, beta_im, direc[c, x])
                    image[c, x] = operated[c, x] - cmul(beta_re, beta_im, image[c, x])

        sums = [jnp.zeros((size, 2 * half), jnp.float32) for _ in range(4)]
        for c in range(3):
            for x in range(planes):
                d, m, r = direc[c, x], image[c, x], res_out[c, x]
                td = turn(d)
                sums[0] = sums[0] + d * m
                sums[1] = sums[1] + td * m
                sums[2] = sums[2] + d * r
                sums[3] = sums[3] + td * r
        for i in range(4):
            part_send[2 * it + 1, i : i + 1] = folded(sums[i])
        part_start(2 * it + 1)
        return carry

    part_send[...] = jnp.zeros_like(part_send)
    lax.fori_loop(0, ITERS, iteration, 0)
    update(*solve(*gram_totals(ITERS)))
    for c in range(3):
        for x in range(planes):
            emit(sol_flat, sol_out, c, x)
            emit(res_flat, res_out, c, x)


def on_device(right_side, material, permittivity, bloch_phase, quad_shift):
    planes = right_side.shape[3]
    count = lax.axis_size("px")
    size = planes * count
    lanes = 2 * size
    groups = size // 2
    pad = -(-2 * planes // 8) * 8
    f32 = jnp.float32

    def flat(value):
        lead = value.shape[:-2]
        value = value.reshape(lead + (planes, groups, lanes))
        return jnp.swapaxes(value, -3, -2).reshape(lead + (groups * planes, lanes))

    def restored(value):
        value = value.reshape(2, 3, groups, planes, lanes)
        return jnp.swapaxes(value, -3, -2).reshape(right_side.shape)

    vmem = pl.BlockSpec(memory_space=pltpu.VMEM)
    smem = pl.BlockSpec(memory_space=pltpu.SMEM)
    plane = (size, lanes)
    field = pltpu.VMEM((3, planes) + plane, f32)
    planar = pltpu.VMEM((planes,) + plane, f32)
    exchanged = pltpu.VMEM((2 * ITERS, 3, count * pad, lanes), f32)
    extended = pltpu.VMEM((3, planes + 2) + plane, f32)
    rows = (pad, lanes)
    dma = pltpu.SemaphoreType.DMA
    out = jax.ShapeDtypeStruct((2, 3, groups * planes, lanes), f32)
    solved, left = pl.pallas_call(
        functools.partial(kernel_body, count, planes, size, pad, permittivity.shape[0]),
        out_shape=(out, out),
        in_specs=[smem] * 3 + [vmem] * 2,
        out_specs=(vmem, vmem),
        scratch_shapes=[
            field,
            field,
            planar,
            pltpu.VMEM((lanes, 2 * lanes), f32),
            pltpu.VMEM(plane, f32),
            pltpu.VMEM((lanes, 2 * lanes), f32),
            pltpu.VMEM(plane, f32),
            pltpu.VMEM((2,) + rows, f32),
            pltpu.VMEM((2,) + plane, f32),
            pltpu.VMEM(plane, f32),
            pltpu.VMEM(plane, f32),
            pltpu.VMEM(plane, f32),
            pltpu.VMEM((count + 1,) + rows, f32),
            pltpu.VMEM((2,) + rows, f32),
            field,
            extended,
            pltpu.VMEM((planes + 2,) + plane, f32),
            pltpu.VMEM((ITERS,) + plane, f32),
            exchanged,
            exchanged,
            extended,
            field,
            field,
            pltpu.VMEM((3, planes + 1) + plane, f32),
            field,
            pltpu.VMEM(plane, f32),
            pltpu.VMEM(plane, f32),
            planar,
            pltpu.VMEM((2 * ITERS, 8, lanes), f32),
            pltpu.VMEM((2 * ITERS, count, 8, lanes), f32),
            dma((2, 3, count)),
            dma((2, 3, count)),
            dma((2, count)),
            dma((2, count)),
            dma((1 + ITERS,)),
            dma((1 + ITERS,)),
        ],
        compiler_params=pltpu.CompilerParams(
            collective_id=0, has_side_effects=True, vmem_limit_bytes=60 * 2**20
        ),
    )(permittivity, bloch_phase, quad_shift, flat(right_side[:, :, 0]), flat(material))
    return restored(solved), restored(left)


def solution(mesh):
    return jax.shard_map(
        on_device,
        mesh=mesh,
        in_specs=(P(None, None, "kpt", "px", None), P("px", None), P(), P("kpt"), P()),
        out_specs=(P(None, None, "kpt", "px", None), P(None, None, "kpt", "px", None)),
        check_vma=False,
    )
```

```python
import functools
import math

import jax
import jax.numpy as jnp
from jax import lax
from jax.experimental import pallas as pl
from jax.experimental.pallas import tpu as pltpu
from jax.sharding import PartitionSpec as P

ITERS = 3
PRECISE = lax.Precision.HIGH
MESH = pl.DeviceIdType.MESH


def dot(a, b):
    return lax.dot_general(
        a, b, (((1,), (0,)), ((), ())), precision=PRECISE, preferred_element_type=jnp.float32
    )


def kernel_body(
    count,
    planes,
    size,
    pad,
    kinds,
    permittivity,
    bloch,
    shift,
    right,
    material,
    sol_flat,
    res_flat,
    sol_out,
    res_out,
    permit,
    rzf,
    lyf,
    rzi,
    lyi,
    lanes,
    dy,
    decay,
    green,
    middle,
    own_decay,
    wrap,
    spec,
    solved,
    inner_buf,
    low_spec,
    send,
    recv,
    precond,
    direc,
    image,
    curl_buf,
    operated,
    low_permit,
    inv_low,
    inv_eps,
    part_send,
    part_recv,
    a2a_send_sem,
    a2a_recv_sem,
    part_send_sem,
    part_recv_sem,
    halo_send_sem,
    halo_recv_sem,
):
    me = lax.axis_index("px")
    kys = size // count
    chunk = pad
    half = size

    def peer(k):
        return lax.rem(me + k, count)

    barrier = pltpu.get_barrier_semaphore()

    def greet(k, carry):
        pl.semaphore_signal(
            barrier, inc=1, device_id={"px": peer(k)}, device_id_type=MESH
        )
        return carry

    lax.fori_loop(1, count, greet, 0)

    def turn(f):
        return pltpu.roll(f, half, f.ndim - 1) * sign

    def cmul(re, im, f):
        return re * f + im * turn(f)

    def copy_to(src, dst, ssem, rsem, target):
        return pltpu.make_async_remote_copy(
            src_ref=src,
            dst_ref=dst,
            send_sem=ssem,
            recv_sem=rsem,
            device_id={"px": target},
            device_id_type=MESH,
        )

    def rows(dev):
        return pl.ds(pl.multiple_of(dev * chunk, 8), chunk)

    def exchange_copy(e, par, c, k):
        return copy_to(
            send.at[e, c, rows(peer(k))],
            recv.at[e, c, rows(me)],
            a2a_send_sem.at[par, c, k],
            a2a_recv_sem.at[par, c, k],
            peer(k),
        )

    def exchange_start(e, par, c):
        def start(k, carry):
            exchange_copy(e, par, c, k).start()
            return carry

        lax.fori_loop(1, count, start, 0)
        recv[e, c, rows(me), :] = send[e, c, rows(me), :]

    def exchange_finish(e, par, c):
        def finish(k, carry):
            exchange_copy(e, par, c, k).wait()
            return carry

        lax.fori_loop(1, count, finish, 0)

    def part_copy(e, k):
        return copy_to(
            part_send.at[e],
            part_recv.at[e, me],
            part_send_sem.at[lax.rem(e, 2), k],
            part_recv_sem.at[lax.rem(e, 2), k],
            peer(k),
        )

    def part_start(e):
        def start(k, carry):
            part_copy(e, k).start()
            return carry

        lax.fori_loop(1, count, start, 0)
        part_recv[e, me] = part_send[e]

    def part_finish(e):
        def finish(k, carry):
            part_copy(e, k).wait()
            return carry

        lax.fori_loop(1, count, finish, 0)
        total = part_recv[e, 0]
        for s in range(1, count):
            total = total + part_recv[e, s]
        return jnp.sum(total, axis=1, keepdims=True)


    wide = (size, 2 * half)
    row = lax.broadcasted_iota(jnp.int32, wide, 0)
    lane = lax.broadcasted_iota(jnp.int32, wide, 1)
    low = lane < half
    index = jnp.where(low, lane, lane - half)
    quarter = jnp.where(low, 0.0, 0.5 * math.pi)
    minus_high = jnp.where(low, 1.0, -1.0)
    minus_low = -minus_high
    base = (2.0 * math.pi / size) * lax.rem(row * index, size).astype(jnp.float32) - quarter
    sign = minus_low[0:1]

    def swap(f):
        return pltpu.roll(f, half, 1)

    def by_mode(axis):
        return jnp.cos(base + bloch[axis] * index.astype(jnp.float32) / size)

    def by_cell(axis):
        return jnp.cos(base + bloch[axis] * row.astype(jnp.float32) / size)

    lyf[...] = by_mode(1) * minus_high
    lyi[...] = by_cell(1) / size
    cells = by_cell(2)
    rzf[0:half, 0 : 2 * half] = cells * minus_high
    rzf[0:half, 2 * half :] = swap(cells)
    rzf[half:, 0 : 2 * half] = swap(cells)
    rzf[half:, 2 * half :] = cells * minus_low
    modes = by_mode(2) / size
    rzi[0:half, 0 : 2 * half] = modes
    rzi[0:half, 2 * half :] = swap(modes) * minus_low
    rzi[half:, 0 : 2 * half] = swap(modes) * minus_low
    rzi[half:, 2 * half :] = -modes

    kappa_y = (2.0 * math.pi * row.astype(jnp.float32) + bloch[1]) / size
    dy[0] = jnp.cos(kappa_y) - 1.0
    dy[1] = jnp.sin(kappa_y)
    short = (lanes.shape[1], 2 * half)
    line = lax.broadcasted_iota(jnp.int32, short, 0)
    place = lax.broadcasted_iota(jnp.int32, short, 1)
    place = jnp.where(place < half, place, place - half)
    angles = (2.0 * math.pi * place.astype(jnp.float32) + bloch[2]) / size
    for axis in range(3):
        angles = jnp.where(line == axis, bloch[axis], angles)
    my_ky = (me * kys + lax.rem(line, kys)).astype(jnp.float32)
    my_kappa = (2.0 * math.pi * my_ky + bloch[1]) / size
    lanes[0] = jnp.cos(angles)
    lanes[1] = jnp.sin(angles)

    def wave(i):
        return lanes[0, i : i + 1, :], lanes[1, i : i + 1, :]

    def difference(i):
        return lanes[0, i : i + 1, :] - 1.0, lanes[1, i : i + 1, :]

    mean = permittivity[0]
    for i in range(1, kinds):
        mean = mean + permittivity[i]
    damping = jnp.full((1, 2 * half), shift[0] * mean * (1.0 / kinds), jnp.float32)
    over_damping = 1.0 / damping
    dz_re, dz_im = difference(3)
    square_z = dz_re**2 + dz_im**2 + damping

    def decay_of(sigma):
        root = jnp.sqrt(sigma + 0.25 * sigma * sigma)
        return 1.0 / (1.0 + 0.5 * sigma + root), 0.5 / root

    sigma = dy[0] ** 2 + dy[1] ** 2 + square_z
    lam, green_value = decay_of(sigma)
    decay[...] = lam
    green[...] = green_value
    middle[...] = 2.0 + sigma
    my_square = (jnp.cos(my_kappa) - 1.0) ** 2 + jnp.sin(my_kappa) ** 2
    my_lam, _ = decay_of(my_square + square_z)
    my_step = my_lam
    for _ in range(planes - 1):
        my_step = my_step * my_lam
    power = jnp.ones(short, jnp.float32)
    for s in range(count):
        own_decay[s] = power
        power = power * my_step
    own_decay[count] = power
    is_low = line < kys
    cos_x, sin_x = wave(0)
    bottom = 1.0 / (1.0 - 2.0 * power * cos_x + power * power)
    wrap[0] = (cos_x - power) * bottom
    wrap[1] = jnp.where(is_low, -sin_x, sin_x) * bottom

    (cos_y, sin_y), (cos_z, sin_z) = wave(1), wave(2)
    cos_dn = jnp.where(me == 0, cos_x, 1.0)
    sin_dn = jnp.where(me == 0, -sin_x, 0.0)
    index_row, low_row = index[0:1], low[0:1]
    last, first = index_row == size - 1, index_row == 0
    zfa = jnp.where(last, jnp.where(low_row, -sin_z, sin_z), 1.0)
    zfb = jnp.where(last, cos_z, 0.0)
    zba = jnp.where(first, jnp.where(low_row, sin_z, -sin_z), 1.0)
    zbb = jnp.where(first, cos_z, 0.0)
    q0, q1 = shift[0], shift[1]

    half_low = low[0 : size // 2]

    def every(x):
        return pl.ds(x, size // 2, stride=planes)

    even, odd = pl.ds(0, size // 2, stride=2), pl.ds(1, size // 2, stride=2)
    for x in range(planes):
        kind = material[every(x), :]
        scaled = jnp.zeros(kind.shape, jnp.float32)
        for i in range(kinds):
            scaled = scaled + jnp.where(kind == i, permittivity[i], jnp.float32(0.0))
        turned = swap(scaled)
        permit[x, even, :] = jnp.where(half_low, scaled, turned)
        permit[x, odd, :] = jnp.where(half_low, turned, scaled)
        for c in range(3):
            re, im = right[0, c, every(x), :], right[1, c, every(x), :]
            res_out[c, x, even, :] = jnp.where(half_low, re, swap(im))
            res_out[c, x, odd, :] = jnp.where(half_low, swap(re), im)

    def emit(flat, field, c, x):
        a, b = field[c, x, even, :], field[c, x, odd, :]
        flat[0, c, every(x), :] = jnp.where(half_low, a, swap(b))
        flat[1, c, every(x), :] = jnp.where(half_low, swap(a), b)

    pl.semaphore_wait(barrier, count - 1)

    permit_copy = copy_to(
        permit.at[planes - 1],
        low_permit,
        halo_send_sem.at[0],
        halo_recv_sem.at[0],
        peer(1),
    )
    permit_copy.start()
    inv_eps[...] = 1.0 / permit[...]

    def plane_copy(it):
        return copy_to(
            spec.at[0, planes - 1],
            low_spec.at[it],
            halo_send_sem.at[1 + it],
            halo_recv_sem.at[1 + it],
            peer(1),
        )

    def spectrum_forward(e, c):
        lam = decay[...]
        up = down = None
        for x in range(planes):
            both = dot(image[c, x], rzf[...])
            mixed = jnp.concatenate([both[:, : 2 * half], both[:, 2 * half :]], 0)
            out = dot(lyf[...], mixed)
            spec[c, x] = out
            if x == 0:
                up = down = out
                power = lam
            else:
                up = up * lam + out
                down = down + out * power
                power = power * lam
        for d in range(count):
            at = d * chunk
            send[e, c, at : at + kys, :] = up[d * kys : (d + 1) * kys, :]
            send[e, c, at + kys : at + 2 * kys, :] = down[d * kys : (d + 1) * kys, :]

    def scan(e, c):
        step = own_decay[1]
        below, above = [jnp.zeros(short, jnp.float32)], [jnp.zeros(short, jnp.float32)]
        for s in range(count):
            t = count - 1 - s
            below.append(below[-1] * step + recv[e, c, s * chunk : (s + 1) * chunk, :])
            above.append(above[-1] * step + recv[e, c, t * chunk : (t + 1) * chunk, :])
        total = cmul(wrap[0], wrap[1], jnp.where(is_low, below[-1], above[-1]))
        for d in range(count):
            t = count - 1 - d
            value = jnp.where(is_low, below[d], above[t])
            power = jnp.where(is_low, own_decay[d], own_decay[t])
            send[e + 1, c, d * chunk : (d + 1) * chunk, :] = value + power * total

    def column_solve(e, c):
        for s in range(count):
            at = s * chunk
            inner_buf[0, s * kys : (s + 1) * kys, :] = recv[e + 1, c, at : at + kys, :]
            inner_buf[1, s * kys : (s + 1) * kys, :] = recv[
                e + 1, c, at + kys : at + 2 * kys, :
            ]
        lam, scale = decay[...], green[...]
        total = inner_buf[0]
        solved[c, 0] = total
        for x in range(planes):
            total = total * lam + spec[c, x]
            solved[c, x + 1] = total
        total = inner_buf[1]
        solved[c, planes + 1] = (solved[c, planes] * lam + total) * scale
        for x in range(planes - 1, -2, -1):
            total = total * lam
            solved[c, x + 1] = (solved[c, x + 1] + total) * scale
            if x >= 0:
                total = total + spec[c, x]

    def couple(it):
        dy_re, dy_im = dy[0], dy[1]
        low = cmul(cos_dn, sin_dn, low_spec[it])
        prior = middle[...] * solved[0, 0] - solved[0, 1] - low
        for x in range(planes + 2):
            here = solved[0, x]
            term = prior - here
            prior = here
            for c, (re, im) in ((1, (dy_re, dy_im)), (2, difference(3))):
                f = solved[c, x]
                term = term + re * f - im * turn(f)
            inner_buf[x] = term * over_damping
        for x in range(planes + 2):
            if x <= planes:
                solved[0, x] = solved[0, x] + (inner_buf[x + 1] - inner_buf[x])
            inner = inner_buf[x]
            turned = turn(inner)
            solved[1, x] = solved[1, x] + dy_re * inner + dy_im * turned
            dz_re, dz_im = difference(3)
            solved[2, x] = solved[2, x] + dz_re * inner + dz_im * turned

    def field_back(c, x):
        both = dot(solved[c, x], rzi[...])
        mixed = jnp.concatenate([both[:, : 2 * half], both[:, 2 * half :]], 0)
        return dot(lyi[...], mixed)

    def wide_planes(c):
        return planes + (1 if c == 0 else 2)

    def next_y(f):
        edge = cmul(cos_y, sin_y, f[0:1])
        return jnp.where(row == size - 1, edge, pltpu.roll(f, size - 1, 0))

    def prev_y(f):
        edge = cmul(cos_y, -sin_y, f[size - 1 : size])
        return jnp.where(row == 0, edge, pltpu.roll(f, 1, 0))

    def next_z(f):
        return pltpu.roll(f, 2 * half - 1, 1) * zfa + pltpu.roll(f, half - 1, 1) * zfb

    def prev_z(f):
        return pltpu.roll(f, 1, 1) * zba + pltpu.roll(f, half + 1, 1) * zbb

    def operate():
        for x in range(-1, planes):
            e = [precond[c, x + 1] for c in range(3)]
            inv = inv_low[...] if x < 0 else inv_eps[x]
            up_y, up_z = precond[1, x + 2], precond[2, x + 2]
            curl_buf[1, x + 1] = ((next_z(e[0]) - e[0]) - (up_z - e[2])) * inv
            curl_buf[2, x + 1] = ((up_y - e[1]) - (next_y(e[0]) - e[0])) * inv
            if x >= 0:
                curl_buf[0, x + 1] = (
                    (next_y(e[2]) - e[2]) - (next_z(e[1]) - e[1])
                ) * inv
        for x in range(planes):
            h = [curl_buf[c, x + 1] for c in range(3)]
            low_y, low_z = curl_buf[1, x], curl_buf[2, x]
            parts = [
                (prev_z(h[1]) - h[1]) - (prev_y(h[2]) - h[2]),
                (low_z - h[2]) - (prev_z(h[0]) - h[0]),
                (prev_y(h[0]) - h[0]) - (low_y - h[1]),
            ]
            for c in range(3):
                operated[c, x] = parts[c] + cmul(q0, q1, precond[c, x + 1]) * permit[x]

    def solve(g_re, g_im, s_re, s_im):
        factor = g_im / g_re
        low = (s_im - factor * s_re) / (g_re + factor * g_im)
        return (s_re + g_im * low) / g_re, low

    def folded(value):
        return jnp.sum(value, axis=0, keepdims=True)

    image[...] = res_out[...]
    sol_out[...] = jnp.zeros_like(sol_out)
    direc[...] = jnp.zeros_like(direc)

    def update(coef_re, coef_im):
        for c in range(3):
            for x in range(planes):
                sol_out[c, x] = sol_out[c, x] + cmul(coef_re, coef_im, direc[c, x])
                res_out[c, x] = res_out[c, x] - cmul(coef_re, coef_im, image[c, x])

    def gram_totals(it):
        totals = part_finish(2 * it - 1)
        return totals[0:1], totals[1:2], totals[2:3], totals[3:4]

    def iteration(it, carry):
        e = 2 * it
        for c in range(3):
            spectrum_forward(e, c)
            exchange_start(e, 0, c)
            if c == 0:
                plane_copy(it).start()
        for c in range(3):
            exchange_finish(e, 0, c)
            scan(e, c)
            exchange_start(e + 1, 1, c)
        for c in range(3):
            exchange_finish(e + 1, 1, c)
            column_solve(e, c)
        plane_copy(it).wait()
        couple(it)

        @pl.when(it == 0)
        def _():
            for c in range(3):
                for x in range(wide_planes(c)):
                    precond[c, x] = field_back(c, x)
            permit_copy.wait()
            inv_low[...] = 1.0 / low_permit[...]
            operate()
            for c in range(3):
                for x in range(planes):
                    direc[c, x] = precond[c, x + 1]
                    image[c, x] = operated[c, x]

        @pl.when(it > 0)
        def _():
            g_re, g_im, s_re, s_im = gram_totals(it)
            coef_re, coef_im = solve(g_re, g_im, s_re, s_im)
            sum_re = jnp.zeros((size, 2 * half), jnp.float32)
            sum_im = jnp.zeros((size, 2 * half), jnp.float32)
            for c in range(3):
                for x in range(wide_planes(c)):
                    value = precond[c, x] - cmul(coef_re, coef_im, field_back(c, x))
                    precond[c, x] = value
                    if 1 <= x <= planes:
                        sum_re = sum_re + image[c, x - 1] * value
                        sum_im = sum_im - image[c, x - 1] * turn(value)
            part_send[2 * it, 0:1] = folded(sum_re)
            part_send[2 * it, 1:2] = folded(sum_im)
            part_start(2 * it)
            update(coef_re, coef_im)
            operate()
            totals = part_finish(2 * it)
            beta_re, beta_im = solve(g_re, g_im, totals[0:1], totals[1:2])
            for c in range(3):
                for x in range(planes):
                    direc[c, x] = precond[c, x + 1] - cmul(beta_re, beta_im, direc[c, x])
                    image[c, x] = operated[c, x] - cmul(beta_re, beta_im, image[c, x])

        sums = [jnp.zeros((size, 2 * half), jnp.float32) for _ in range(4)]
        for c in range(3):
            for x in range(planes):
                d, m, r = direc[c, x], image[c, x], res_out[c, x]
                td = turn(d)
                sums[0] = sums[0] + d * m
                sums[1] = sums[1] + td * m
                sums[2] = sums[2] + d * r
                sums[3] = sums[3] + td * r
        for i in range(4):
            part_send[2 * it + 1, i : i + 1] = folded(sums[i])
        part_start(2 * it + 1)
        return carry

    part_send[...] = jnp.zeros_like(part_send)
    lax.fori_loop(0, ITERS, iteration, 0)
    update(*solve(*gram_totals(ITERS)))
    for c in range(3):
        for x in range(planes):
            emit(sol_flat, sol_out, c, x)
            emit(res_flat, res_out, c, x)


def on_device(right_side, material, permittivity, bloch_phase, quad_shift):
    planes = right_side.shape[3]
    count = lax.axis_size("px")
    size = planes * count
    lanes = 2 * size
    groups = size // 2
    pad = -(-2 * planes // 8) * 8
    f32 = jnp.float32

    def flat(value):
        lead = value.shape[:-2]
        value = value.reshape(lead + (planes, groups, lanes))
        return jnp.swapaxes(value, -3, -2).reshape(lead + (groups * planes, lanes))

    def restored(value):
        value = value.reshape(2, 3, groups, planes, lanes)
        return jnp.swapaxes(value, -3, -2).reshape(right_side.shape)

    vmem = pl.BlockSpec(memory_space=pltpu.VMEM)
    smem = pl.BlockSpec(memory_space=pltpu.SMEM)
    plane = (size, lanes)
    field = pltpu.VMEM((3, planes) + plane, f32)
    planar = pltpu.VMEM((planes,) + plane, f32)
    exchanged = pltpu.VMEM((2 * ITERS, 3, count * pad, lanes), f32)
    extended = pltpu.VMEM((3, planes + 2) + plane, f32)
    rows = (pad, lanes)
    dma = pltpu.SemaphoreType.DMA
    out = jax.ShapeDtypeStruct((2, 3, groups * planes, lanes), f32)
    solved, left = pl.pallas_call(
        functools.partial(kernel_body, count, planes, size, pad, permittivity.shape[0]),
        out_shape=(out, out),
        in_specs=[smem] * 3 + [vmem] * 2,
        out_specs=(vmem, vmem),
        scratch_shapes=[
            field,
            field,
            planar,
            pltpu.VMEM((lanes, 2 * lanes), f32),
            pltpu.VMEM(plane, f32),
            pltpu.VMEM((lanes, 2 * lanes), f32),
            pltpu.VMEM(plane, f32),
            pltpu.VMEM((2,) + rows, f32),
            pltpu.VMEM((2,) + plane, f32),
            pltpu.VMEM(plane, f32),
            pltpu.VMEM(plane, f32),
            pltpu.VMEM(plane, f32),
            pltpu.VMEM((count + 1,) + rows, f32),
            pltpu.VMEM((2,) + rows, f32),
            field,
            extended,
            pltpu.VMEM((planes + 2,) + plane, f32),
            pltpu.VMEM((ITERS,) + plane, f32),
            exchanged,
            exchanged,
            extended,
            field,
            field,
            pltpu.VMEM((3, planes + 1) + plane, f32),
            field,
            pltpu.VMEM(plane, f32),
            pltpu.VMEM(plane, f32),
            planar,
            pltpu.VMEM((2 * ITERS, 8, lanes), f32),
            pltpu.VMEM((2 * ITERS, count, 8, lanes), f32),
            dma((2, 3, count)),
            dma((2, 3, count)),
            dma((2, count)),
            dma((2, count)),
            dma((1 + ITERS,)),
            dma((1 + ITERS,)),
        ],
        compiler_params=pltpu.CompilerParams(
            collective_id=0, has_side_effects=True, vmem_limit_bytes=60 * 2**20
        ),
    )(permittivity, bloch_phase, quad_shift, flat(right_side[:, :, 0]), flat(material))
    return restored(solved), restored(left)


def solution(mesh):
    return jax.shard_map(
        on_device,
        mesh=mesh,
        in_specs=(P(None, None, "kpt", "px", None), P("px", None), P(), P("kpt"), P()),
        out_specs=(P(None, None, "kpt", "px", None), P(None, None, "kpt", "px", None)),
        check_vma=False,
    )
```
